16 devices in a mesh: rep: 1, dp: 16 (over x, y, z, core).
Axes of the slice: x: 2, y: 2, z: 2, core: 2. Of those that a mesh axis runs over, the one named last changes fastest.
Arguments:
- x: bfloat16 [16, 2048, 768], P(('rep', 'dp'))
- dy: bfloat16 [16, 2048, 768], P(('rep', 'dp'))
- w_gate: bfloat16 [2, 768, 3072], replicated
- w_up: bfloat16 [2, 768, 3072], replicated
- w_down: bfloat16 [2, 3072, 768], replicated
- m_w_gate: float32 [2, 768, 3072], P(None, 'dp')
- m_w_up: float32 [2, 768, 3072], P(None, 'dp')
- m_w_down: float32 [2, 3072, 768], P(None, 'dp')
- v_w_gate: float32 [2, 768, 3072], P(None, 'dp')
- v_w_up: float32 [2, 768, 3072], P(None, 'dp')
- v_w_down: float32 [2, 3072, 768], P(None, 'dp')
Outputs:
- output 1: bfloat16 [2, 768, 3072], P('rep')
- output 2: bfloat16 [2, 768, 3072], P('rep')
- output 3: bfloat16 [2, 3072, 768], P('rep')
- output 4: float32 [2, 768, 3072], P('rep', 'dp')
- output 5: float32 [2, 768, 3072], P('rep', 'dp')
- output 6: float32 [2, 3072, 768], P('rep', 'dp')
- output 7: float32 [2, 768, 3072], P('rep', 'dp')
- output 8: float32 [2, 768, 3072], P('rep', 'dp')
- output 9: float32 [2, 3072, 768], P('rep', 'dp')
All inputs are finite; a program needn't handle non-finite values.
Results may differ from the reference program's by a relative error of at most 0.022.
Values are sent between devices in bfloat16 or wider.
A program may use at most 2 GiB of HBM per device.

```python
import jax
import jax.numpy as jnp
from jax import lax

SEQUENCES = 16
TOKENS = 2048
D = 768
FF = 3072
LAYERS = 2
NAMES = ("w_gate", "w_up", "w_down")
SHAPES = {"w_gate": (LAYERS, D, FF), "w_up": (LAYERS, D, FF), "w_down": (LAYERS, FF, D)}


def bump(key, n, height):
    away = (jnp.arange(n, dtype=jnp.int32) - jax.random.randint(key, (), 0, n, jnp.int32)) % n
    return jnp.where(away < n // 8, height, 1.0)


def together(key, own, strength):
    shared = jax.random.normal(key, own.shape[1:], jnp.float32)
    return (own + strength * shared) * lax.rsqrt(1 + strength * strength)


def setup_inputs(seed: int = 0, part: int = 0) -> dict:
    kx, kdy, ka, kb, kz, kf, kh, kl, *keys = jax.random.split(jax.random.key(seed), 8 + 3 * len(NAMES))
    kx, kdy, ka, kb = (jax.random.fold_in(k, part) for k in (kx, kdy, ka, kb))
    kw, km, kv = (keys[i::3] for i in range(3))
    shape = (SEQUENCES, TOKENS, D)
    much_x, much_dy = jax.random.uniform(kz, (2,), jnp.float32, 0.0, 1.0)
    loud = 2.0 ** jax.random.uniform(jax.random.fold_in(kz, 1), (), jnp.float32, -1.0, 2.0)
    layers = 2.0 ** jax.random.uniform(kl, (LAYERS, 1, 1), jnp.float32, -1.0, 1.0)
    x = together(ka, jax.random.normal(kx, shape, jnp.float32), much_x) * bump(kf, D, 4.0)
    dy = together(kb, jax.random.normal(kdy, shape, jnp.float32), much_dy)
    drawn = {"x": x.astype(jnp.bfloat16), "dy": (loud * dy * (SEQUENCES * TOKENS) ** -0.5).astype(jnp.bfloat16)}
    for key, name in zip(kw, NAMES, strict=True):
        w = jax.random.normal(key, SHAPES[name], jnp.float32) * SHAPES[name][1] ** -0.5
        drawn[name] = (w * {"w_gate": 1.0, "w_up": bump(kh, FF, 4.0), "w_down": layers}[name]).astype(jnp.bfloat16)
    for key, name in zip(km, NAMES, strict=True):
        drawn[f"m_{name}"] = 0.1 * jax.random.normal(key, SHAPES[name], jnp.float32)
    for key, name in zip(kv, NAMES, strict=True):
        drawn[f"v_{name}"] = jax.random.uniform(key, SHAPES[name], jnp.float32, 0.005, 0.015)
    return drawn


def matmul(a, w):
    return jnp.dot(a, w, preferred_element_type=jnp.float32).astype(jnp.bfloat16)


def normed(h):
    wide = h.astype(jnp.float32)
    scale = lax.rsqrt(jnp.mean(wide**2, -1, keepdims=True) + 1e-6)
    return (wide * scale).astype(jnp.bfloat16)


def layer(h, w):
    a = normed(h)
    gate = jnp.dot(a, w["w_gate"], preferred_element_type=jnp.float32)
    up = jnp.dot(a, w["w_up"], preferred_element_type=jnp.float32)
    return h + matmul((jax.nn.silu(gate) * up).astype(jnp.bfloat16), w["w_down"])


def adamw(w, m, v, g):
    m = 0.9 * m + 0.1 * g
    v = 0.95 * v + 0.05 * g * g
    step = m * lax.rsqrt(v + 1e-8) + 0.1 * w
    return (w - 0.02 * step).astype(jnp.bfloat16), m, v


def stack(weights, h):
    return lax.scan(lambda h, w: (layer(h, w), None), h, weights)[0]


def reference(x, dy, w_gate, w_up, w_down, m_w_gate, m_w_up, m_w_down, v_w_gate, v_w_up, v_w_down):
    weights = dict(zip(NAMES, (w_gate, w_up, w_down), strict=True))

    def take(so_far, sequence):
        h, by_y = sequence
        _, back = jax.vjp(lambda w: stack(w, h), weights)
        return jax.tree.map(lambda total, term: total + term.astype(jnp.float32), so_far, back(by_y)[0]), None

    none_yet = {name: jnp.zeros(w.shape, jnp.float32) for name, w in weights.items()}
    by_weights, _ = lax.scan(take, none_yet, (x, dy))
    gradients = [by_weights[name].astype(jnp.bfloat16).astype(jnp.float32) for name in NAMES]
    new = [
        adamw(w.astype(jnp.float32), m, v, g)
        for w, m, v, g in zip((w_gate, w_up, w_down), (m_w_gate, m_w_up, m_w_down), (v_w_gate, v_w_up, v_w_down), gradients, strict=True)
    ]
    return tuple(one[which] for which in range(3) for one in new)
```

```python
import jax
import jax.numpy as jnp
from jax import lax
from jax.sharding import PartitionSpec as P


def dot(a, b, dims=((1,), (0,))):
    return lax.dot_general(a, b, (dims, ((), ())), preferred_element_type=jnp.float32)


def scale_of(h):
    wide = h.astype(jnp.float32)
    return lax.rsqrt(jnp.mean(wide * wide, -1, keepdims=True) + 1e-6)


def adamw(w, m, v, g):
    m = 0.9 * m + 0.1 * g
    v = 0.95 * v + 0.05 * g * g
    step = m * lax.rsqrt(v + 1e-8) + 0.1 * w
    return (w - 0.02 * step).astype(jnp.bfloat16), m, v


def hidden(gate, up):
    return (jax.nn.silu(gate) * up).astype(jnp.bfloat16)


def back_of_hidden(gate, up, d_s):
    d_s = d_s.astype(jnp.float32)
    sig = jax.nn.sigmoid(gate)
    d_up = d_s * gate * sig
    d_gate = d_s * up * sig * (1 + gate * (1 - sig))
    return d_gate.astype(jnp.bfloat16), d_up.astype(jnp.bfloat16)


def back_of_norm(h, scale, d_a):
    wide, d_a = h.astype(jnp.float32), d_a.astype(jnp.float32)
    dot_ = jnp.mean(d_a * wide, -1, keepdims=True)
    return (d_a * scale - wide * (scale * scale * scale * dot_)).astype(jnp.bfloat16)


def solution(mesh):
    n = mesh.shape["dp"]

    def step(x, dy, wg, wu, wd, mg, mu, md, vg, vu, vd):
        x, dy = x[0], dy[0]
        bf = jnp.bfloat16
        r0 = scale_of(x)
        a0 = (x.astype(jnp.float32) * r0).astype(bf)
        gate0, up0 = dot(a0, wg[0]), dot(a0, wu[0])
        s0 = hidden(gate0, up0)
        h1 = x + dot(s0, wd[0]).astype(bf)
        r1 = scale_of(h1)
        a1 = (h1.astype(jnp.float32) * r1).astype(bf)
        gate1, up1 = dot(a1, wg[1]), dot(a1, wu[1])
        s1 = hidden(gate1, up1)
        g = {}

        def grad(a, b):
            return dot(a, b, ((0,), (0,))).astype(bf)

        def update(name, layer, term, w, m, v):
            total = lax.psum_scatter(term, "dp", scatter_dimension=0, tiled=True).astype(jnp.float32)
            rows = term.shape[0] // n
            mine = lax.dynamic_slice_in_dim(w[layer], lax.axis_index("dp") * rows, rows)
            nw, nm, nv = adamw(mine.astype(jnp.float32), m[layer], v[layer], total)
            g[name, layer] = (lax.all_gather(nw, "dp", axis=0, tiled=True), nm, nv)

        update("d", 1, grad(s1, dy), wd, md, vd)
        ds1 = dot(dy, wd[1], ((1,), (1,))).astype(bf)
        dg1, du1 = back_of_hidden(gate1, up1, ds1)
        update("g", 1, grad(a1, dg1), wg, mg, vg)
        update("u", 1, grad(a1, du1), wu, mu, vu)
        da1 = dot(dg1, wg[1], ((1,), (1,))).astype(bf) + dot(du1, wu[1], ((1,), (1,))).astype(bf)
        dh1 = dy + back_of_norm(h1, r1, da1)
        update("d", 0, grad(s0, dh1), wd, md, vd)
        ds0 = dot(dh1, wd[0], ((1,), (1,))).astype(bf)
        dg0, du0 = back_of_hidden(gate0, up0, ds0)
        update("g", 0, grad(a0, dg0), wg, mg, vg)
        update("u", 0, grad(a0, du0), wu, mu, vu)
        return tuple(jnp.stack([g[name, 0][k], g[name, 1][k]]) for k in range(3) for name in "gud")

    whole, rows = P(None, None, None), P(None, "dp", None)
    return jax.shard_map(
        step,
        mesh=mesh,
        in_specs=(P(("rep", "dp")), P(("rep", "dp")), *[whole] * 3, *[rows] * 6),
        out_specs=(*[P("rep", None, None)] * 3, *[P("rep", "dp", None)] * 6),
        check_vma=False,
    )
```

```python
import jax
import jax.numpy as jnp
from jax import lax
from jax.experimental import pallas as pl
from jax.experimental.pallas import tpu as pltpu
from jax.sharding import PartitionSpec as P

F32, BF16 = jnp.float32, jnp.bfloat16
MESH = pl.DeviceIdType.MESH
D, FF, TOKENS, TILE, WIDE = 768, 3072, 2048, 512, 1024
PIECES = FF // WIDE
ROWS = D // 16
CHUNKS = 18
SLOTS = 8
MIB = 2**20


def dot(a, b, dims=((1,), (0,))):
    return lax.dot_general(a, b, (dims, ((), ())), preferred_element_type=F32)


NT, TN = ((1,), (1,)), ((0,), (0,))


def scale_of(wide):
    return lax.rsqrt(jnp.mean(wide * wide, -1, keepdims=True) + 1e-6)


def back_of_hidden(gate, up, d_s):
    sig = 1 / (1 + jnp.exp(-gate))
    silu = gate * sig
    d_up = d_s * silu
    d_gate = d_s * up * (sig + silu * (1 - sig))
    return silu * up, d_gate, d_up


def adamw(w, m, v, g):
    m = 0.9 * m + 0.1 * g
    v = 0.95 * v + 0.05 * g * g
    step = m * lax.rsqrt(v + 1e-8) + 0.1 * w
    return (w - 0.02 * step).astype(BF16), m, v


def forward_kernel(x, wg, wu, wd, a_out, gate_out, up_out, s_out, h_out):
    wide = x[...].astype(F32)
    a = (wide * scale_of(wide)).astype(BF16)
    a_out[...] = a
    for c in range(PIECES):
        at = slice(c * WIDE, (c + 1) * WIDE)
        gate, up = dot(a, wg[:, at]), dot(a, wu[:, at])
        gate_out[:, at] = gate
        up_out[:, at] = up
        s_out[:, at] = (gate / (1 + jnp.exp(-gate)) * up).astype(BF16)
    h_out[...] = x[...] + dot(s_out[...], wd[...]).astype(BF16)


def turn_kernel(h, dy, wg, wu, wd, a_out, s_out, dg_out, du_out, dh_out):
    wide = h[...].astype(F32)
    scale = scale_of(wide)
    a = (wide * scale).astype(BF16)
    a_out[...] = a
    for c in range(PIECES):
        at = slice(c * WIDE, (c + 1) * WIDE)
        gate, up = dot(a, wg[:, at]), dot(a, wu[:, at])
        d_s = dot(dy[...], wd[at, :], NT).astype(BF16).astype(F32)
        s, d_gate, d_up = back_of_hidden(gate, up, d_s)
        s_out[:, at] = s.astype(BF16)
        dg_out[:, at] = d_gate.astype(BF16)
        du_out[:, at] = d_up.astype(BF16)
    d_a = dot(dg_out[...], wg[...], NT).astype(BF16) + dot(du_out[...], wu[...], NT).astype(BF16)
    d_a = d_a.astype(F32)
    along = jnp.mean(d_a * wide, -1, keepdims=True)
    dh_out[...] = dy[...] + (d_a * scale - wide * (scale * scale * scale * along)).astype(BF16)


def back_kernel(dh, gate, up, wd, dg_out, du_out):
    for c in range(PIECES):
        at = slice(c * WIDE, (c + 1) * WIDE)
        d_s = dot(dh[...], wd[at, :], NT).astype(BF16).astype(F32)
        _, d_gate, d_up = back_of_hidden(gate[:, at], up[:, at], d_s)
        dg_out[:, at] = d_gate.astype(BF16)
        du_out[:, at] = d_up.astype(BF16)


def by_tiles(kernel, ins, weights, layer, outs, flops):
    def tile(width):
        return pl.BlockSpec((TILE, width), lambda i: (i, 0))

    def whole(w):
        return pl.BlockSpec((None, *w.shape[1:]), lambda i: (layer, 0, 0), pipeline_mode=pl.Buffered(1))

    return pl.pallas_call(
        kernel,
        grid=(TOKENS // TILE,),
        in_specs=[tile(t.shape[1]) for t in ins] + [whole(w) for w in weights],
        out_specs=[tile(width) for width, _ in outs],
        out_shape=[jax.ShapeDtypeStruct((TOKENS, width), dtype) for width, dtype in outs],
        compiler_params=pltpu.CompilerParams(vmem_limit_bytes=62 * MIB),
        cost_estimate=pl.CostEstimate(flops=flops, bytes_accessed=50 * MIB, transcendentals=0),
    )(*ins, *weights)


def sum_kernel(*refs):
    (a1, a0, s1, s0, dy, dh1, dg1, du1, dg0, du0, wg, wu, wd, mg, mu, md, vg, vu, vd) = refs[:19]
    (nwg, nwu, nwd, nmg, nmu, nmd, nvg, nvu, nvd) = refs[19:28]
    (a_in, s_in, rhs, part, r0, q, r1, r2, r3, new, m_in, v_in, w_in, m_out, v_out) = refs[28:43]
    (sem_a, sem_s, sem_rhs, sem_mv, sem_mvo, sem_out, x0, x1, x2, x3, g1, g2, g3, g4) = refs[43:]

    me = lax.axis_index("dp")
    pos = [me // 8, (me // 4) % 2, (me // 2) % 2]
    core = me % 2
    mate = [me + 8 - 16 * pos[0], me + 4 - 8 * pos[1], me + 2 - 4 * pos[2]]
    twin = me + 1 - 2 * core

    barrier = pltpu.get_barrier_semaphore()
    for other in (*mate, twin):
        pl.semaphore_signal(barrier, inc=1, device_id=(0, other), device_id_type=MESH)
    pl.semaphore_wait(barrier, 4)

    def remote(src, dst, sems, index, to):
        return pltpu.make_async_remote_copy(
            src_ref=src,
            dst_ref=dst,
            send_sem=sems.at[(0, *index)],
            recv_sem=sems.at[(1, *index)],
            device_id=(0, to),
            device_id_type=MESH,
        )

    def at(chosen):
        return tuple(chosen.get(axis, slice(None)) for axis in range(3))

    def which(k):
        return 1 - k // 9, (k % 9) // 3, k % 3

    def swap0(k):
        return remote(part.at[k % 2, :, :, :, 1 - core], r0.at[k % 2], x0, (k % 2,), twin)

    def rows(r):
        return pl.ds(16 * r, 16)

    def swap1(k, r):
        a = r
        src = q.at[(k % 3, *at({a: 1 - pos[a]}), rows(r))]
        return remote(src, r1.at[k % 2, r], x1, (k % 2, r), mate[a])

    def swap2(k, r):
        a, b = r, (r + 1) % 3
        src = q.at[(k % 3, *at({a: pos[a], b: 1 - pos[b]}), rows(r))]
        return remote(src, r2.at[k % 2, r], x2, (k % 2, r), mate[b])

    def swap3(k, r):
        a, b, c = r, (r + 1) % 3, (r + 2) % 3
        src = q.at[(k % 3, *at({a: pos[a], b: pos[b], c: 1 - pos[c]}), rows(r))]
        return remote(src, r3.at[k % 2, r], x3, (k % 2, r), mate[c])

    def give(k, r, known, sems, axis):
        ref = new.at[(k % SLOTS, *at({n: pos[n] for n in known}), core, rows(r))]
        return remote(ref, ref, sems, (k % 2, r), mate[axis])

    def give1(k, r):
        return give(k, r, (0, 1, 2), g1, (r + 2) % 3)

    def give2(k, r):
        return give(k, r, (r, (r + 1) % 3), g2, (r + 1) % 3)

    def give3(k, r):
        return give(k, r, (r,), g3, r)

    def give4(k):
        ref = new.at[k % SLOTS, :, :, :, core]
        return remote(ref, ref, g4, (k % 2,), twin)

    def operand(k, act):
        layer, kind, j = which(k)
        cols = pl.ds(pl.multiple_of(j * WIDE, 128), WIDE)
        few = pl.ds(pl.multiple_of(j * 256, 128), 256)
        n = 0
        for at_layer, sources in ((1, (dg1, du1, dy)), (0, (dg0, du0, dh1))):
            for at_kind, src in enumerate(sources):

                @pl.when((layer == at_layer) & (kind == at_kind))
                def _(src=src, at_kind=at_kind):
                    if at_kind < 2:
                        act(pltpu.make_async_copy(src.at[:, cols], rhs.at[k % 2], sem_rhs.at[k % 2]))
                    else:
                        act(pltpu.make_async_copy(src.at[:, few], rhs.at[k % 2, :, pl.ds(0, 256)], sem_rhs.at[k % 2]))

    def state(k, act, back):
        layer, kind, j = which(k)
        cols = pl.ds(pl.multiple_of(j * WIDE, 128), WIDE)
        few = pl.ds(pl.multiple_of(j * 256, 128), 256)
        for at_kind, (w, m, v, nm, nv) in enumerate(((wg, mg, vg, nmg, nvg), (wu, mu, vu, nmu, nvu), (wd, md, vd, nmd, nvd))):

            @pl.when(kind == at_kind)
            def _(w=w, m=m, v=v, nm=nm, nv=nv, at_kind=at_kind):
                if at_kind < 2:
                    if back:
                        act(pltpu.make_async_copy(m_out, nm.at[layer, :, cols], sem_mvo.at[0, 0]))
                        act(pltpu.make_async_copy(v_out, nv.at[layer, :, cols], sem_mvo.at[1, 0]))
                    else:
                        act(pltpu.make_async_copy(m.at[layer, :, cols], m_in, sem_mv.at[0, 0]))
                        act(pltpu.make_async_copy(v.at[layer, :, cols], v_in, sem_mv.at[1, 0]))
                        act(pltpu.make_async_copy(w.at[layer, me, :, cols], w_in, sem_mv.at[2, 0]))
                else:
                    for n in range(4):
                        here = pl.ds(256 * n, 256)
                        if back:
                            act(pltpu.make_async_copy(m_out.at[:, here], nm.at[layer, n, :, few], sem_mvo.at[0, n]))
                            act(pltpu.make_async_copy(v_out.at[:, here], nv.at[layer, n, :, few], sem_mvo.at[1, n]))
                        else:
                            act(pltpu.make_async_copy(m.at[layer, n, :, few], m_in.at[:, here], sem_mv.at[0, n]))
                            act(pltpu.make_async_copy(v.at[layer, n, :, few], v_in.at[:, here], sem_mv.at[1, n]))
                            act(pltpu.make_async_copy(w.at[layer, me, n, :, few], w_in.at[:, here], sem_mv.at[2, n]))

    def result(k, act):
        layer, kind, j = which(k)
        cols = pl.ds(pl.multiple_of(j * WIDE, 128), WIDE)
        few = pl.ds(pl.multiple_of(j * 256, 128), 256)
        for at_kind, out in enumerate((nwg, nwu, nwd)):

            @pl.when(kind == at_kind)
            def _(out=out, at_kind=at_kind):
                if at_kind < 2:
                    act(pltpu.make_async_copy(new.at[k % SLOTS], out.at[layer, :, :, :, :, :, cols], sem_out.at[k % 2, 0]))
                else:
                    for n in range(4):
                        src = new.at[k % SLOTS, :, :, :, :, :, pl.ds(256 * n, 256)]
                        act(pltpu.make_async_copy(src, out.at[layer, :, :, :, :, n, :, few], sem_out.at[k % 2, n]))

    def start(copy):
        copy.start()

    def wait(copy):
        copy.wait()

    def load_a(src):
        return pltpu.make_async_copy(src, a_in, sem_a.at[0])

    def load_s(src):
        return pltpu.make_async_copy(src, s_in, sem_s.at[0])

    load_a(a1).start()
    operand(0, start)
    load_s(s1).start()

    def step(i, carry):
        slot = i % 2

        @pl.when(i < CHUNKS)
        def _():
            operand(i, wait)

            @pl.when(i + 1 < CHUNKS)
            def _():
                operand(i + 1, start)

            @pl.when(i == 0)
            def _():
                load_a(a1).wait()

            @pl.when(i == 6)
            def _():
                load_a(a0).start()
                load_s(s1).wait()

            @pl.when(i == 9)
            def _():
                load_a(a0).wait()
                load_s(s0).start()

            @pl.when(i == 15)
            def _():
                load_s(s0).wait()

            kind = (i % 9) // 3

            @pl.when(kind < 2)
            def _():
                term = dot(a_in[...], rhs[slot], TN).astype(BF16)
                part[slot] = term.reshape(2, 2, 2, 2, ROWS, WIDE)

            @pl.when(kind == 2)
            def _():
                term = dot(s_in[...], rhs[slot, :, :256], TN).astype(BF16)
                term = term.reshape(2, 2, 2, 2, 4, ROWS, 256)
                for n in range(4):
                    part[slot, :, :, :, :, :, pl.ds(256 * n, 256)] = term[:, :, :, :, n]

        def stage(back, body):
            @pl.when((i >= back) & (i < CHUNKS + back))
            def _():
                body(i - back)

        @stage_with(stage, 9)
        def _(k):
            result(k, wait)

        @stage_with(stage, 8)
        def _(k):
            give4(k).wait()
            result(k, start)

        @stage_with(stage, 7)
        def _(k):
            for r in range(3):
                give3(k, r).wait()
            give4(k).start()

        @stage_with(stage, 6)
        def _(k):
            for r in range(3):
                give2(k, r).wait()
                give3(k, r).start()

        @stage_with(stage, 5)
        def _(k):
            state(k, wait, True)
            for r in range(3):
                give1(k, r).wait()
                give2(k, r).start()

        @stage_with(stage, 4)
        def _(k):
            state(k, wait, False)
            for r in range(3):
                swap3(k, r).wait()
                mine = (k % 3, *pos, rows(r))
                total = (q[mine].astype(F32) + r3[k % 2, r].astype(F32)).astype(BF16).astype(F32)
                w, m, v = adamw(w_in[rows(r), :].astype(F32), m_in[rows(r), :], v_in[rows(r), :], total)
                m_out[rows(r), :] = m
                v_out[rows(r), :] = v
                new[(k % SLOTS, *pos, core, rows(r))] = w
            for r in range(3):
                give1(k, r).start()
            state(k, start, True)

        @stage_with(stage, 3)
        def _(k):
            state(k, start, False)
            for r in range(3):
                a, b = r, (r + 1) % 3
                swap2(k, r).wait()
                mine = (k % 3, *at({a: pos[a], b: pos[b]}), rows(r))
                q[mine] = (q[mine].astype(F32) + r2[k % 2, r].astype(F32)).astype(BF16)
            for r in range(3):
                swap3(k, r).start()

        @stage_with(stage, 2)
        def _(k):
            for r in range(3):
                swap1(k, r).wait()
                mine = (k % 3, *at({r: pos[r]}), rows(r))
                q[mine] = (q[mine].astype(F32) + r1[k % 2, r].astype(F32)).astype(BF16)
            for r in range(3):
                swap2(k, r).start()

        @stage_with(stage, 1)
        def _(k):
            swap0(k).wait()
            for n in range(2):
                mine = part[k % 2, n, :, :, core].astype(F32) + r0[k % 2, n].astype(F32)
                q[k % 3, n] = mine.astype(BF16)
            for r in range(3):
                swap1(k, r).start()

        @pl.when(i < CHUNKS)
        def _():
            swap0(i).start()

        return carry

    lax.fori_loop(0, CHUNKS + 10, step, 0)


def stage_with(stage, back):
    return lambda body: stage(back, body)


def sum_and_step(ins, wg, wu, wd, mg, mu, md, vg, vu, vd):
    dims = (2, 2, 2, 2, 2)
    any_ = pl.BlockSpec(memory_space=pl.ANY)
    wg, wu = (w.reshape(2, 16, ROWS, FF) for w in (wg, wu))
    wd = wd.reshape(2, 16, 4, ROWS, D)
    md, vd = (t.reshape(2, 4, ROWS, D) for t in (md, vd))
    vmem = pltpu.VMEM
    dma = pltpu.SemaphoreType.DMA
    outs = pl.pallas_call(
        sum_kernel,
        in_specs=[any_] * 19,
        out_specs=[any_] * 9,
        out_shape=[jax.ShapeDtypeStruct((*dims, ROWS, FF), BF16)] * 2
        + [jax.ShapeDtypeStruct((*dims, 4, ROWS, D), BF16)]
        + ([jax.ShapeDtypeStruct((2, ROWS, FF), F32)] * 2 + [jax.ShapeDtypeStruct((2, 4, ROWS, D), F32)]) * 2,
        scratch_shapes=[
            vmem((TOKENS, D), BF16),
            vmem((TOKENS, FF), BF16),
            vmem((2, TOKENS, WIDE), BF16),
            vmem((2, 2, 2, 2, 2, ROWS, WIDE), BF16),
            vmem((2, 2, 2, 2, ROWS, WIDE), BF16),
            vmem((3, 2, 2, 2, ROWS, WIDE), BF16),
            vmem((2, 3, 2, 2, 16, WIDE), BF16),
            vmem((2, 3, 2, 16, WIDE), BF16),
            vmem((2, 3, 16, WIDE), BF16),
            vmem((SLOTS, 2, 2, 2, 2, ROWS, WIDE), BF16),
            vmem((ROWS, WIDE), F32),
            vmem((ROWS, WIDE), F32),
            vmem((ROWS, WIDE), BF16),
            vmem((ROWS, WIDE), F32),
            vmem((ROWS, WIDE), F32),
            dma((1,)),
            dma((1,)),
            dma((2,)),
            dma((3, 4)),
            dma((2, 4)),
            dma((2, 4)),
            dma((2, 2)),
            dma((2, 2, 3)),
            dma((2, 2, 3)),
            dma((2, 2, 3)),
            dma((2, 2, 3)),
            dma((2, 2, 3)),
            dma((2, 2, 3)),
            dma((2, 2)),
        ],
        compiler_params=pltpu.CompilerParams(collective_id=0, has_side_effects=True, vmem_limit_bytes=62 * MIB),
        cost_estimate=pl.CostEstimate(flops=6 * 2 * TOKENS * D * FF, bytes_accessed=120 * MIB, transcendentals=0),
    )(*ins, wg, wu, wd, mg, mu, md, vg, vu, vd)
    shapes = [(2, D, FF)] * 2 + [(2, FF, D)] + ([(2, ROWS, FF)] * 2 + [(2, 4 * ROWS, D)]) * 2
    return tuple(t.reshape(shape) for t, shape in zip(outs, shapes, strict=True))


def solution(mesh):
    def step(x, dy, wg, wu, wd, *moments):
        x, dy = x[0], dy[0]
        one = 2 * TOKENS * D * FF
        a0, gate0, up0, s0, h1 = by_tiles(
            forward_kernel, (x,), (wg, wu, wd), 0, ((D, BF16), (FF, F32), (FF, F32), (FF, BF16), (D, BF16)), 3 * one
        )
        a1, s1, dg1, du1, dh1 = by_tiles(
            turn_kernel, (h1, dy), (wg, wu, wd), 1, ((D, BF16), (FF, BF16), (FF, BF16), (FF, BF16), (D, BF16)), 5 * one
        )
        dg0, du0 = by_tiles(back_kernel, (dh1, gate0, up0), (wd,), 0, ((FF, BF16), (FF, BF16)), one)
        return sum_and_step((a1, a0, s1, s0, dy, dh1, dg1, du1, dg0, du0), wg, wu, wd, *moments)

    whole, rows = P(None, None, None), P(None, "dp", None)
    return jax.shard_map(
        step,
        mesh=mesh,
        in_specs=(P(("rep", "dp")), P(("rep", "dp")), *[whole] * 3, *[rows] * 6),
        out_specs=(*[P("rep", None, None)] * 3, *[P("rep", "dp", None)] * 6),
        check_vma=False,
    )
```

```python
import jax
import jax.numpy as jnp
from jax import lax
from jax.experimental import pallas as pl
from jax.experimental.pallas import tpu as pltpu
from jax.sharding import PartitionSpec as P

F32, BF16 = jnp.float32, jnp.bfloat16
MESH = pl.DeviceIdType.MESH
D, FF, TOKENS, TILE, WIDE = 768, 3072, 2048, 512, 1024
PIECES = FF // WIDE
ROWS = D // 16
CHUNKS = 18
SMALL, NARROW = 256, 512
SIXTHS = FF // NARROW
AHEAD = 4
COPIES = 3
MIB = 2**20


def dot(a, b, dims=((1,), (0,))):
    return lax.dot_general(a, b, (dims, ((), ())), preferred_element_type=F32)


NT, TN = ((1,), (1,)), ((0,), (0,))


def scale_of(wide):
    return lax.rsqrt(jnp.mean(wide * wide, -1, keepdims=True) + 1e-6)


def silu_and_slope(gate):
    sig = 0.5 * jnp.tanh(0.5 * gate) + 0.5
    silu = gate * sig
    return silu, 0.5 * (sig + silu * (1 - sig))


def adamw(w, m, v, g):
    m = 0.9 * m + 0.1 * g
    v = 0.95 * v + 0.05 * g * g
    step = m * lax.rsqrt(v + 1e-8) + 0.1 * w
    return (w - 0.02 * step).astype(BF16), m, v


def forward_kernel(x, wg, wu, wd, a_out, silu_out, slope_out, s_out, h_out):
    wide = x[...].astype(F32)
    a = (wide * scale_of(wide)).astype(BF16)
    a_out[...] = a
    for c in range(PIECES):
        at = slice(c * WIDE, (c + 1) * WIDE)
        gate, up = dot(a, wg[:, at]), dot(a, wu[:, at])
        silu, slope = silu_and_slope(gate)
        silu_out[:, at] = silu
        slope_out[:, at] = up * slope
        s_out[:, at] = (silu * up).astype(BF16)
    h_out[...] = x[...] + dot(s_out[...], wd[...]).astype(BF16)


def turn_kernel(h, dy, wg, wu, wd, a_out, s_out, dg_out, du_out):
    wide = h[...].astype(F32)
    a = (wide * scale_of(wide)).astype(BF16)
    a_out[...] = a
    for c in range(PIECES):
        at = slice(c * WIDE, (c + 1) * WIDE)
        gate, up = dot(a, wg[:, at]), dot(a, wu[:, at])
        d_s = dot(dy[...], wd[at, :], NT).astype(BF16).astype(F32)
        silu, slope = silu_and_slope(gate)
        s_out[:, at] = (silu * up).astype(BF16)
        dg_out[:, at] = (d_s * (up * slope) * 2).astype(BF16)
        du_out[:, at] = (d_s * silu).astype(BF16)


def by_tiles(kernel, ins, weights, layer, outs, flops):
    def tile(width):
        return pl.BlockSpec((TILE, width), lambda i: (i, 0))

    def whole(w):
        return pl.BlockSpec((None, *w.shape[1:]), lambda i: (layer, 0, 0), pipeline_mode=pl.Buffered(1))

    return pl.pallas_call(
        kernel,
        grid=(TOKENS // TILE,),
        in_specs=[tile(t.shape[1]) for t in ins] + [whole(w) for w in weights],
        out_specs=[tile(width) for width, _ in outs],
        out_shape=[jax.ShapeDtypeStruct((TOKENS, width), dtype) for width, dtype in outs],
        compiler_params=pltpu.CompilerParams(vmem_limit_bytes=62 * MIB),
        cost_estimate=pl.CostEstimate(flops=flops, bytes_accessed=50 * MIB, transcendentals=0),
    )(*ins, *weights)


def sum_kernel(*refs):
    (a1, a0, s1, s0, dy, h1, dg1, du1, silu0, slope0, wg, wu, wd, mg, mu, md, vg, vu, vd) = refs[:19]
    (nwg, nwu, nwd, nmg, nmu, nmd, nvg, nvu, nvd, dg0, du0) = refs[19:30]
    (a_in, s_in, rhs, part, r0, q, r1, r2, r3, new, new_d, m_in, v_in, w_in, m_out, v_out) = refs[30:46]
    (wg_in, wu_in, wd_in, dh, d_tile, h_tile, kept) = refs[46:53]
    (sem_a, sem_s, sem_rhs, sem_mv, sem_mvo, sem_own, x0, x1, x2, x3, g1, g2, g3, g4, sem_w, sem_tile, sem_kept, sem_d) = refs[53:]

    me = lax.axis_index("dp")
    pos = [me // 8, (me // 4) % 2, (me // 2) % 2]
    core = me % 2
    mate = [me + 8 - 16 * pos[0], me + 4 - 8 * pos[1], me + 2 - 4 * pos[2]]
    twin = me + 1 - 2 * core

    barrier = pltpu.get_barrier_semaphore()
    for other in (*mate, twin):
        pl.semaphore_signal(barrier, inc=1, device_id=(0, other), device_id_type=MESH)
    pl.semaphore_wait(barrier, 4)

    def remote(src, dst, sems, index, to):
        return pltpu.make_async_remote_copy(
            src_ref=src,
            dst_ref=dst,
            send_sem=sems.at[(0, *index)],
            recv_sem=sems.at[(1, *index)],
            device_id=(0, to),
            device_id_type=MESH,
        )

    def at(chosen):
        return tuple(chosen.get(axis, slice(None)) for axis in range(3))

    def which(k):
        layer, third = 1 - k // 9, k // 3
        return layer, layer * ((2 * third) % 3) + (1 - layer) * ((third + 2) % 3), k % 3

    def swap0(k):
        return remote(part.at[k % 2, :, :, :, 1 - core], r0.at[k % 2], x0, (k % 2,), twin)

    def rows(r):
        return pl.ds(16 * r, 16)

    def swap1(k, r):
        a = r
        src = q.at[(k % 3, *at({a: 1 - pos[a]}), rows(r))]
        return remote(src, r1.at[k % 2, r], x1, (k % 2, r), mate[a])

    def swap2(k, r):
        a, b = r, (r + 1) % 3
        src = q.at[(k % 3, *at({a: pos[a], b: 1 - pos[b]}), rows(r))]
        return remote(src, r2.at[k % 2, r], x2, (k % 2, r), mate[b])

    def swap3(k, r):
        a, b, c = r, (r + 1) % 3, (r + 2) % 3
        src = q.at[(k % 3, *at({a: pos[a], b: pos[b], c: 1 - pos[c]}), rows(r))]
        return remote(src, r3.at[k % 2, r], x3, (k % 2, r), mate[c])

    def by_kind(k, gate_like, down_like):
        layer, kind, j = which(k)
        cols = pl.ds(pl.multiple_of(j * WIDE, 128), WIDE)
        few = pl.ds(pl.multiple_of(j * 256, 128), 256)

        @pl.when(kind == 0)
        def _():
            gate_like(nwg, layer, cols)

        @pl.when(kind == 1)
        def _():
            gate_like(nwu, layer, cols)

        @pl.when(kind == 2)
        def _():
            down_like(nwd, layer, few)

    def give1(k, act):
        def send(r, src, dst):
            act(remote(src, dst, g1, (k % 2, r), mate[(r + 2) % 3]))

        def gate_like(out, layer, cols):
            act(pltpu.make_async_copy(new, out.at[(layer, *pos, core, slice(None), cols)], sem_own.at[0]))
            for r in range(3):
                send(r, new.at[rows(r), :], out.at[(layer, *pos, core, rows(r), cols)])

        def down_like(out, layer, few):
            act(pltpu.make_async_copy(new_d, out.at[(layer, *pos, core, slice(None), slice(None), few)], sem_own.at[0]))
            for r in range(3):
                send(r, new_d.at[:, rows(r), :], out.at[(layer, *pos, core, slice(None), rows(r), few)])

        by_kind(k, gate_like, down_like)

    def give(k, known, sems, axis, act):
        def gate_like(out, layer, cols):
            for r in range(3):
                chips = at({(r + n) % 3: pos[(r + n) % 3] for n in range(known)})
                ref = out.at[(layer, *chips, core, rows(r), cols)]
                act(remote(ref, ref, sems, (k % 2, r), mate[(r + axis) % 3]))

        def down_like(out, layer, few):
            for r in range(3):
                chips = at({(r + n) % 3: pos[(r + n) % 3] for n in range(known)})
                ref = out.at[(layer, *chips, core, slice(None), rows(r), few)]
                act(remote(ref, ref, sems, (k % 2, r), mate[(r + axis) % 3]))

        by_kind(k, gate_like, down_like)

    def give2(k, act):
        give(k, 2, g2, 1, act)

    def give3(k, act):
        give(k, 1, g3, 0, act)

    def give4(k, act):
        def gate_like(out, layer, cols):
            ref = out.at[layer, :, :, :, core, :, cols]
            act(remote(ref, ref, g4, (k % 2,), twin))

        def down_like(out, layer, few):
            ref = out.at[layer, :, :, :, core, :, :, few]
            act(remote(ref, ref, g4, (k % 2,), twin))

        by_kind(k, gate_like, down_like)

    def operand(k, act):
        layer, kind, j = which(k)
        cols = pl.ds(pl.multiple_of(j * WIDE, 128), WIDE)
        few = pl.ds(pl.multiple_of(j * 256, 128), 256)
        n = 0
        for at_layer, sources in ((1, (dg1, du1, dy)), (0, (dg0, du0, dh))):
            for at_kind, src in enumerate(sources):

                @pl.when((layer == at_layer) & (kind == at_kind))
                def _(src=src, at_kind=at_kind):
                    if at_kind < 2:
                        act(pltpu.make_async_copy(src.at[:, cols], rhs.at[k % 2], sem_rhs.at[k % 2]))
                    else:
                        act(pltpu.make_async_copy(src.at[:, few], rhs.at[k % 2, :, pl.ds(0, 256)], sem_rhs.at[k % 2]))

    def state(k, act, back):
        layer, kind, j = which(k)
        cols = pl.ds(pl.multiple_of(j * WIDE, 128), WIDE)
        few = pl.ds(pl.multiple_of(j * 256, 128), 256)
        for at_kind, (w, m, v, nm, nv) in enumerate(((wg, mg, vg, nmg, nvg), (wu, mu, vu, nmu, nvu), (wd, md, vd, nmd, nvd))):

            @pl.when(kind == at_kind)
            def _(w=w, m=m, v=v, nm=nm, nv=nv, at_kind=at_kind):
                if at_kind < 2:
                    if back:
                        act(pltpu.make_async_copy(m_out, nm.at[layer, :, cols], sem_mvo.at[0, 0]))
                        act(pltpu.make_async_copy(v_out, nv.at[layer, :, cols], sem_mvo.at[1, 0]))
                    else:
                        act(pltpu.make_async_copy(m.at[layer, :, cols], m_in, sem_mv.at[0, 0]))
                        act(pltpu.make_async_copy(v.at[layer, :, cols], v_in, sem_mv.at[1, 0]))
                        act(pltpu.make_async_copy(w.at[layer, pl.ds(pl.multiple_of(me * ROWS, 16), ROWS), cols], w_in, sem_mv.at[2, 0]))
                else:
                    for n in range(4):
                        here = pl.ds(256 * n, 256)
                        if back:
                            act(pltpu.make_async_copy(m_out.at[:, here], nm.at[layer, n, :, few], sem_mvo.at[0, n]))
                            act(pltpu.make_async_copy(v_out.at[:, here], nv.at[layer, n, :, few], sem_mvo.at[1, n]))
                        else:
                            act(pltpu.make_async_copy(m.at[layer, n, :, few], m_in.at[:, here], sem_mv.at[0, n]))
                            act(pltpu.make_async_copy(v.at[layer, n, :, few], v_in.at[:, here], sem_mv.at[1, n]))
                            own = pl.ds(pl.multiple_of((4 * me + n) * ROWS, 16), ROWS)
                            act(pltpu.make_async_copy(w.at[layer, own, few], w_in.at[:, here], sem_mv.at[2, n]))

    def start(copy):
        copy.start()

    def wait(copy):
        copy.wait()

    def load_a(src):
        return pltpu.make_async_copy(src, a_in, sem_a.at[0])

    def load_s(src):
        return pltpu.make_async_copy(src, s_in, sem_s.at[0])

    def tile(t, act):
        here = pl.ds(pl.multiple_of(t * SMALL, SMALL), SMALL)
        for n, src in enumerate((dg1, du1)):
            act(pltpu.make_async_copy(src.at[here, :], d_tile.at[n], sem_tile.at[n]))
        for n, src in enumerate((h1, dy)):
            act(pltpu.make_async_copy(src.at[here, :], h_tile.at[n], sem_tile.at[2 + n]))

    def hidden(n, act):
        here = pl.ds(pl.multiple_of((n // SIXTHS) * SMALL, SMALL), SMALL)
        cols = pl.ds(pl.multiple_of((n % SIXTHS) * NARROW, 128), NARROW)
        for m, src in enumerate((silu0, slope0)):
            act(pltpu.make_async_copy(src.at[here, cols], kept.at[n % AHEAD, m], sem_kept.at[n % AHEAD, m]))

    def back(t, act):
        here = pl.ds(pl.multiple_of(t * SMALL, SMALL), SMALL)
        for n, out in enumerate((dg0, du0)):
            act(pltpu.make_async_copy(d_tile.at[n], out.at[here, :], sem_d.at[n]))

    def load_w(n):
        src, dst = ((wg.at[1], wg_in), (wu.at[1], wu_in), (wd.at[0], wd_in))[n]
        return pltpu.make_async_copy(src, dst, sem_w.at[n])

    load_a(a1).start()
    operand(0, start)
    tile(0, start)
    load_w(0).start()
    load_w(1).start()
    load_s(s1).start()
    load_w(2).start()
    for n in range(AHEAD):
        hidden(n, start)

    def step(i, carry):
        slot = i % 2

        @pl.when(i < CHUNKS)
        def _():
            operand(i, wait)

            @pl.when((i + 1 < CHUNKS) & (i != 11))
            def _():
                operand(i + 1, start)

            @pl.when(i == 0)
            def _():
                load_a(a1).wait()

            @pl.when(i == 3)
            def _():
                load_s(s1).wait()

            @pl.when(i == 6)
            def _():
                load_s(s0).start()

            @pl.when(i == 9)
            def _():
                load_a(a0).start()
                load_s(s0).wait()

            @pl.when(i == 12)
            def _():
                load_a(a0).wait()

            _, kind, _ = which(i)

            @pl.when(kind < 2)
            def _():
                term = dot(a_in[...], rhs[slot], TN).astype(BF16)
                part[slot] = term.reshape(2, 2, 2, 2, ROWS, WIDE)

            @pl.when(kind == 2)
            def _():
                for x in range(2):
                    term = dot(s_in[:, x * (FF // 2) : (x + 1) * (FF // 2)], rhs[slot, :, :256], TN).astype(BF16)
                    term = term.reshape(2, 2, 2, 4, ROWS, 256)
                    for n in range(4):
                        part[slot, x, :, :, :, :, pl.ds(256 * n, 256)] = term[:, :, :, n]

        @pl.when((i >= 5) & (i < 12))
        def _():
            back(i - 5, wait)

        @pl.when((i >= 1) & (i < 8))
        def _():
            tile(i, start)

        def stage(back, body):
            @pl.when((i >= back) & (i < CHUNKS + back))
            def _():
                body(i - back)

        @stage_with(stage, 8)
        def _(k):
            give4(k, wait)

        @stage_with(stage, 7)
        def _(k):
            give3(k, wait)
            give4(k, start)

        @stage_with(stage, 6)
        def _(k):
            give2(k, wait)
            give3(k, start)

        @stage_with(stage, 5)
        def _(k):
            state(k, wait, True)
            give1(k, wait)
            give2(k, start)

        @stage_with(stage, 4)
        def _(k):
            state(k, wait, False)
            for r in range(3):
                swap3(k, r).wait()
                mine = (k % 3, *pos, rows(r))
                total = (q[mine].astype(F32) + r3[k % 2, r].astype(F32)).astype(BF16).astype(F32)
                w, m, v = adamw(w_in[rows(r), :].astype(F32), m_in[rows(r), :], v_in[rows(r), :], total)
                m_out[rows(r), :] = m
                v_out[rows(r), :] = v
                new[rows(r), :] = w
                for n in range(4):
                    new_d[n, rows(r), :] = w[:, 256 * n : 256 * n + 256]
            give1(k, start)
            state(k, start, True)

        @stage_with(stage, 3)
        def _(k):
            state(k, start, False)
            for r in range(3):
                a, b = r, (r + 1) % 3
                swap2(k, r).wait()
                mine = (k % 3, *at({a: pos[a], b: pos[b]}), rows(r))
                q[mine] = (q[mine].astype(F32) + r2[k % 2, r].astype(F32)).astype(BF16)
            for r in range(3):
                swap3(k, r).start()

        @stage_with(stage, 2)
        def _(k):
            for r in range(3):
                swap1(k, r).wait()
                mine = (k % 3, *at({r: pos[r]}), rows(r))
                q[mine] = (q[mine].astype(F32) + r1[k % 2, r].astype(F32)).astype(BF16)
            for r in range(3):
                swap2(k, r).start()

        @stage_with(stage, 1)
        def _(k):
            swap0(k).wait()
            for n in range(2):
                mine = part[k % 2, n, :, :, core].astype(F32) + r0[k % 2, n].astype(F32)
                q[k % 3, n] = mine.astype(BF16)
            for r in range(3):
                swap1(k, r).start()

        @pl.when(i < CHUNKS)
        def _():
            swap0(i).start()

        @pl.when(i < 8)
        def _():
            tile(i, wait)

            @pl.when(i == 0)
            def _():
                load_w(0).wait()
                load_w(1).wait()

            d_a = dot(d_tile[0], wg_in[...], NT).astype(BF16) + dot(d_tile[1], wu_in[...], NT).astype(BF16)
            d_a = d_a.astype(F32)
            wide = h_tile[0].astype(F32)
            scale = scale_of(wide)
            along = jnp.mean(d_a * wide, -1, keepdims=True)
            d_h = (d_a * scale - wide * (scale * scale * scale * along)).astype(BF16)
            dh[pl.ds(pl.multiple_of(i * SMALL, SMALL), SMALL), :] = h_tile[1] + d_h

        @pl.when((i >= 4) & (i < 12))
        def _():
            @pl.when(i == 4)
            def _():
                load_w(2).wait()

            t = i - 4
            here = pl.ds(pl.multiple_of(t * SMALL, SMALL), SMALL)
            for p in range(SIXTHS):
                n = SIXTHS * t + p
                cols = slice(p * NARROW, (p + 1) * NARROW)
                hidden(n, wait)
                d_s = dot(dh[here, :], wd_in[cols, :], NT).astype(BF16).astype(F32)
                d_tile[0, :, cols] = (d_s * kept[n % AHEAD, 1] * 2).astype(BF16)
                d_tile[1, :, cols] = (d_s * kept[n % AHEAD, 0]).astype(BF16)

                @pl.when(n + AHEAD < 8 * SIXTHS)
                def _(n=n):
                    hidden(n + AHEAD, start)

            back(t, start)

        @pl.when(i == 11)
        def _():
            back(7, wait)
            operand(12, start)

        return carry

    lax.fori_loop(0, CHUNKS + 8, step, 0)


def stage_with(stage, back):
    return lambda body: stage(back, body)


def sum_and_step(ins, wg, wu, wd, mg, mu, md, vg, vu, vd):
    dims = (2, 2, 2, 2, 2)
    any_ = pl.BlockSpec(memory_space=pl.ANY)
    md, vd = (t.reshape(2, 4, ROWS, D) for t in (md, vd))
    vmem = pltpu.VMEM
    dma = pltpu.SemaphoreType.DMA
    outs = pl.pallas_call(
        sum_kernel,
        in_specs=[any_] * 19,
        out_specs=[any_] * 11,
        out_shape=[jax.ShapeDtypeStruct((*dims, ROWS, FF), BF16)] * 2
        + [jax.ShapeDtypeStruct((*dims, 4, ROWS, D), BF16)]
        + ([jax.ShapeDtypeStruct((2, ROWS, FF), F32)] * 2 + [jax.ShapeDtypeStruct((2, 4, ROWS, D), F32)]) * 2
        + [jax.ShapeDtypeStruct((TOKENS, FF), BF16)] * 2,
        scratch_shapes=[
            vmem((TOKENS, D), BF16),
            vmem((TOKENS, FF), BF16),
            vmem((2, TOKENS, WIDE), BF16),
            vmem((2, 2, 2, 2, 2, ROWS, WIDE), BF16),
            vmem((2, 2, 2, 2, ROWS, WIDE), BF16),
            vmem((3, 2, 2, 2, ROWS, WIDE), BF16),
            vmem((2, 3, 2, 2, 16, WIDE), BF16),
            vmem((2, 3, 2, 16, WIDE), BF16),
            vmem((2, 3, 16, WIDE), BF16),
            vmem((ROWS, WIDE), BF16),
            vmem((4, ROWS, 256), BF16),
            vmem((ROWS, WIDE), F32),
            vmem((ROWS, WIDE), F32),
            vmem((ROWS, WIDE), BF16),
            vmem((ROWS, WIDE), F32),
            vmem((ROWS, WIDE), F32),
            vmem((D, FF), BF16),
            vmem((D, FF), BF16),
            vmem((FF, D), BF16),
            vmem((TOKENS, D), BF16),
            vmem((2, SMALL, FF), BF16),
            vmem((2, SMALL, D), BF16),
            vmem((AHEAD, 2, SMALL, NARROW), F32),
            dma((1,)),
            dma((1,)),
            dma((2,)),
            dma((3, 4)),
            dma((2, 4)),
            dma((1,)),
            dma((2, 2)),
            *[dma((2, 2, 3))] * 6,
            dma((2, 2)),
            dma((3,)),
            dma((4,)),
            dma((AHEAD, 2)),
            dma((2,)),
        ],
        compiler_params=pltpu.CompilerParams(collective_id=0, has_side_effects=True, vmem_limit_bytes=67043328),
        cost_estimate=pl.CostEstimate(flops=9 * 2 * TOKENS * D * FF, bytes_accessed=120 * MIB, transcendentals=0),
    )(*ins, wg, wu, wd, mg, mu, md, vg, vu, vd)
    shapes = [(2, D, FF)] * 2 + [(2, FF, D)] + ([(2, ROWS, FF)] * 2 + [(2, 4 * ROWS, D)]) * 2
    return copied([t.reshape(shape) for t, shape in zip(outs[:9], shapes, strict=True)])


def copy_kernel(*refs):
    n = len(refs) // 2
    for src, dst in zip(refs[:n], refs[n:], strict=True):
        dst[...] = src[...]


def copied(arrays):
    specs = [pl.BlockSpec((None, t.shape[1] // COPIES, t.shape[2]), lambda i: (i // COPIES, i % COPIES, 0)) for t in arrays]
    return tuple(
        pl.pallas_call(
            copy_kernel,
            grid=(2 * COPIES,),
            in_specs=specs,
            out_specs=specs,
            out_shape=[jax.ShapeDtypeStruct(t.shape, t.dtype) for t in arrays],
            compiler_params=pltpu.CompilerParams(vmem_limit_bytes=62 * MIB),
        )(*arrays)
    )


def solution(mesh):
    def step(x, dy, wg, wu, wd, *moments):
        x, dy = x[0], dy[0]
        one = 2 * TOKENS * D * FF
        a0, silu0, slope0, s0, h1 = by_tiles(
            forward_kernel, (x,), (wg, wu, wd), 0, ((D, BF16), (FF, F32), (FF, F32), (FF, BF16), (D, BF16)), 3 * one
        )
        a1, s1, dg1, du1 = by_tiles(
            turn_kernel, (h1, dy), (wg, wu, wd), 1, ((D, BF16), (FF, BF16), (FF, BF16), (FF, BF16)), 3 * one
        )
        return sum_and_step((a1, a0, s1, s0, dy, h1, dg1, du1, silu0, slope0), wg, wu, wd, *moments)

    whole, rows = P(None, None, None), P(None, "dp", None)
    return jax.shard_map(
        step,
        mesh=mesh,
        in_specs=(P(("rep", "dp")), P(("rep", "dp")), *[whole] * 3, *[rows] * 6),
        out_specs=(*[P("rep", None, None)] * 3, *[P("rep", "dp", None)] * 6),
        check_vma=False,
    )
```

```python
import jax
import jax.numpy as jnp
from jax import lax
from jax.experimental import pallas as pl
from jax.experimental.pallas import tpu as pltpu
from jax.sharding import PartitionSpec as P

F32, BF16 = jnp.float32, jnp.bfloat16
MESH = pl.DeviceIdType.MESH
D, FF, TOKENS, TILE, WIDE = 768, 3072, 2048, 512, 1024
ROWS = D // 16
CHUNKS = 18
SMALL, NARROW = 256, 512
SIXTHS = FF // NARROW
AHEAD = 4
COPIES = 3
MIB = 2**20


def dot(a, b, dims=((1,), (0,))):
    return lax.dot_general(a, b, (dims, ((), ())), preferred_element_type=F32)


NT, TN = ((1,), (1,)), ((0,), (0,))


def scale_of(wide):
    return lax.rsqrt(jnp.mean(wide * wide, -1, keepdims=True) + 1e-6)


def silu_and_slope(gate):
    sig = 0.5 * jnp.tanh(0.5 * gate) + 0.5
    silu = gate * sig
    return silu, 0.5 * (sig + silu * (1 - sig))


def adamw(w, m, v, g):
    m = 0.9 * m + 0.1 * g
    v = 0.95 * v + 0.05 * g * g
    step = m * lax.rsqrt(v + 1e-8) + 0.1 * w
    return (w - 0.02 * step).astype(BF16), m, v


def forward_kernel(x, wg, wu, wd, a_out, silu_out, slope_out, s_out, h_out, held):
    i = pl.program_id(0)

    @pl.when(i == 0)
    def _():
        for n in range(0, TOKENS, TILE):
            wide = x[n : n + TILE, :].astype(F32)
            a_out[n : n + TILE, :] = (wide * scale_of(wide)).astype(BF16)

    for n in range(0, TOKENS, TILE):
        here = slice(n, n + TILE)
        gate, up = dot(a_out[here, :], wg[...]), dot(a_out[here, :], wu[...])
        silu, slope = silu_and_slope(gate)
        silu_out[here, :] = silu
        slope_out[here, :] = up * slope
        s = (silu * up).astype(BF16)
        s_out[here, :] = s
        held[here, pl.ds(pl.multiple_of(i * NARROW, NARROW), NARROW)] = s

    @pl.when(i == SIXTHS - 1)
    def _():
        for n in range(0, TOKENS, TILE):
            here = slice(n, n + TILE)
            h_out[here, :] = x[here, :] + dot(held[here, :], wd[...]).astype(BF16)


def turn_kernel(h, dy, wg, wu, wd, a_out, s_out, dg_out, du_out):
    @pl.when(pl.program_id(0) == 0)
    def _():
        for n in range(0, TOKENS, TILE):
            wide = h[n : n + TILE, :].astype(F32)
            a_out[n : n + TILE, :] = (wide * scale_of(wide)).astype(BF16)

    for n in range(0, TOKENS, TILE):
        here = slice(n, n + TILE)
        gate, up = dot(a_out[here, :], wg[...]), dot(a_out[here, :], wu[...])
        d_s = dot(dy[here, :], wd[...], NT).astype(BF16).astype(F32)
        silu, slope = silu_and_slope(gate)
        s_out[here, :] = (silu * up).astype(BF16)
        dg_out[here, :] = (d_s * (up * slope) * 2).astype(BF16)
        du_out[here, :] = (d_s * silu).astype(BF16)


def by_columns(kernel, ins, weights, layer, outs, whole_down, scratch):
    whole = pl.BlockSpec((TOKENS, D), lambda i: (0, 0), pipeline_mode=pl.Buffered(1))
    across = pl.BlockSpec((None, D, NARROW), lambda i: (layer, 0, i))
    if whole_down:
        down = pl.BlockSpec((None, FF, D), lambda i: (layer, 0, 0), pipeline_mode=pl.Buffered(1))
    else:
        down = pl.BlockSpec((None, NARROW, D), lambda i: (layer, i, 0))
    columns = pl.BlockSpec((TOKENS, NARROW), lambda i: (0, i))
    return pl.pallas_call(
        kernel,
        grid=(SIXTHS,),
        in_specs=[whole] * len(ins) + [across, across, down],
        out_specs=[whole if width == D else columns for width, _ in outs],
        out_shape=[jax.ShapeDtypeStruct((TOKENS, width), dtype) for width, dtype in outs],
        scratch_shapes=scratch,
        compiler_params=pltpu.CompilerParams(vmem_limit_bytes=63 * MIB),
        cost_estimate=pl.CostEstimate(flops=6 * TOKENS * D * FF, bytes_accessed=60 * MIB, transcendentals=0),
    )(*ins, *weights)


def sum_kernel(*refs):
    (a1, a0, s1, s0, dy, h1, dg1, du1, silu0, slope0, wg, wu, wd, mg, mu, md, vg, vu, vd) = refs[:19]
    (nwg, nwu, nwd, nmg, nmu, nmd, nvg, nvu, nvd, dg0, du0) = refs[19:30]
    (a_in, s_in, rhs, part, r0, q, r1, r2, r3, new, new_d, m_in, v_in, w_in, m_out, v_out) = refs[30:46]
    (wg_in, wu_in, wd_in, dh, d_tile, h_tile, kept) = refs[46:53]
    (sem_a, sem_s, sem_rhs, sem_mv, sem_mvo, sem_own, x0, x1, x2, x3, g1, g2, g3, g4, sem_w, sem_tile, sem_kept, sem_d) = refs[53:]

    me = lax.axis_index("dp")
    pos = [me // 8, (me // 4) % 2, (me // 2) % 2]
    core = me % 2
    mate = [me + 8 - 16 * pos[0], me + 4 - 8 * pos[1], me + 2 - 4 * pos[2]]
    twin = me + 1 - 2 * core

    barrier = pltpu.get_barrier_semaphore()
    for other in (*mate, twin):
        pl.semaphore_signal(barrier, inc=1, device_id=(0, other), device_id_type=MESH)
    pl.semaphore_wait(barrier, 4)

    def remote(src, dst, sems, index, to):
        return pltpu.make_async_remote_copy(
            src_ref=src,
            dst_ref=dst,
            send_sem=sems.at[(0, *index)],
            recv_sem=sems.at[(1, *index)],
            device_id=(0, to),
            device_id_type=MESH,
        )

    def at(chosen):
        return tuple(chosen.get(axis, slice(None)) for axis in range(3))

    def which(k):
        layer, third = 1 - k // 9, k // 3
        return layer, layer * ((2 * third) % 3) + (1 - layer) * ((third + 2) % 3), k % 3

    def swap0(k):
        return remote(part.at[k % 2, :, :, :, 1 - core], r0.at[k % 2], x0, (k % 2,), twin)

    def rows(r):
        return pl.ds(16 * r, 16)

    def swap1(k, r):
        a = r
        src = q.at[(k % 3, *at({a: 1 - pos[a]}), rows(r))]
        return remote(src, r1.at[k % 2, r], x1, (k % 2, r), mate[a])

    def swap2(k, r):
        a, b = r, (r + 1) % 3
        src = q.at[(k % 3, *at({a: pos[a], b: 1 - pos[b]}), rows(r))]
        return remote(src, r2.at[k % 2, r], x2, (k % 2, r), mate[b])

    def swap3(k, r):
        a, b, c = r, (r + 1) % 3, (r + 2) % 3
        src = q.at[(k % 3, *at({a: pos[a], b: pos[b], c: 1 - pos[c]}), rows(r))]
        return remote(src, r3.at[k % 2, r], x3, (k % 2, r), mate[c])

    def by_kind(k, gate_like, down_like):
        layer, kind, j = which(k)
        cols = pl.ds(pl.multiple_of(j * WIDE, 128), WIDE)
        few = pl.ds(pl.multiple_of(j * 256, 128), 256)

        @pl.when(kind == 0)
        def _():
            gate_like(nwg, layer, cols)

        @pl.when(kind == 1)
        def _():
            gate_like(nwu, layer, cols)

        @pl.when(kind == 2)
        def _():
            down_like(nwd, layer, few)

    def give1(k, act):
        def send(r, src, dst):
            act(remote(src, dst, g1, (k % 2, r), mate[(r + 2) % 3]))

        def gate_like(out, layer, cols):
            act(pltpu.make_async_copy(new, out.at[(layer, *pos, core, slice(None), cols)], sem_own.at[0]))
            for r in range(3):
                send(r, new.at[rows(r), :], out.at[(layer, *pos, core, rows(r), cols)])

        def down_like(out, layer, few):
            act(pltpu.make_async_copy(new_d, out.at[(layer, *pos, core, slice(None), slice(None), few)], sem_own.at[0]))
            for r in range(3):
                send(r, new_d.at[:, rows(r), :], out.at[(layer, *pos, core, slice(None), rows(r), few)])

        by_kind(k, gate_like, down_like)

    def give(k, known, sems, axis, act):
        def gate_like(out, layer, cols):
            for r in range(3):
                chips = at({(r + n) % 3: pos[(r + n) % 3] for n in range(known)})
                ref = out.at[(layer, *chips, core, rows(r), cols)]
                act(remote(ref, ref, sems, (k % 2, r), mate[(r + axis) % 3]))

        def down_like(out, layer, few):
            for r in range(3):
                chips = at({(r + n) % 3: pos[(r + n) % 3] for n in range(known)})
                ref = out.at[(layer, *chips, core, slice(None), rows(r), few)]
                act(remote(ref, ref, sems, (k % 2, r), mate[(r + axis) % 3]))

        by_kind(k, gate_like, down_like)

    def give2(k, act):
        give(k, 2, g2, 1, act)

    def give3(k, act):
        give(k, 1, g3, 0, act)

    def give4(k, act):
        def gate_like(out, layer, cols):
            ref = out.at[layer, :, :, :, core, :, cols]
            act(remote(ref, ref, g4, (k % 2,), twin))

        def down_like(out, layer, few):
            ref = out.at[layer, :, :, :, core, :, :, few]
            act(remote(ref, ref, g4, (k % 2,), twin))

        by_kind(k, gate_like, down_like)

    def operand(k, act):
        layer, kind, j = which(k)
        cols = pl.ds(pl.multiple_of(j * WIDE, 128), WIDE)
        few = pl.ds(pl.multiple_of(j * 256, 128), 256)
        n = 0
        for at_layer, sources in ((1, (dg1, du1, dy)), (0, (dg0, du0, dh))):
            for at_kind, src in enumerate(sources):

                @pl.when((layer == at_layer) & (kind == at_kind))
                def _(src=src, at_kind=at_kind):
                    if at_kind < 2:
                        act(pltpu.make_async_copy(src.at[:, cols], rhs.at[k % 2], sem_rhs.at[k % 2]))
                    else:
                        act(pltpu.make_async_copy(src.at[:, few], rhs.at[k % 2, :, pl.ds(0, 256)], sem_rhs.at[k % 2]))

    def state(k, act, back):
        layer, kind, j = which(k)
        cols = pl.ds(pl.multiple_of(j * WIDE, 128), WIDE)
        few = pl.ds(pl.multiple_of(j * 256, 128), 256)
        for at_kind, (w, m, v, nm, nv) in enumerate(((wg, mg, vg, nmg, nvg), (wu, mu, vu, nmu, nvu), (wd, md, vd, nmd, nvd))):

            @pl.when(kind == at_kind)
            def _(w=w, m=m, v=v, nm=nm, nv=nv, at_kind=at_kind):
                if at_kind < 2:
                    if back:
                        act(pltpu.make_async_copy(m_out, nm.at[layer, :, cols], sem_mvo.at[0, 0]))
                        act(pltpu.make_async_copy(v_out, nv.at[layer, :, cols], sem_mvo.at[1, 0]))
                    else:
                        act(pltpu.make_async_copy(m.at[layer, :, cols], m_in, sem_mv.at[0, 0]))
                        act(pltpu.make_async_copy(v.at[layer, :, cols], v_in, sem_mv.at[1, 0]))
                        act(pltpu.make_async_copy(w.at[layer, pl.ds(pl.multiple_of(me * ROWS, 16), ROWS), cols], w_in, sem_mv.at[2, 0]))
                else:
                    for n in range(4):
                        here = pl.ds(256 * n, 256)
                        if back:
                            act(pltpu.make_async_copy(m_out.at[:, here], nm.at[layer, n, :, few], sem_mvo.at[0, n]))
                            act(pltpu.make_async_copy(v_out.at[:, here], nv.at[layer, n, :, few], sem_mvo.at[1, n]))
                        else:
                            act(pltpu.make_async_copy(m.at[layer, n, :, few], m_in.at[:, here], sem_mv.at[0, n]))
                            act(pltpu.make_async_copy(v.at[layer, n, :, few], v_in.at[:, here], sem_mv.at[1, n]))
                            own = pl.ds(pl.multiple_of((4 * me + n) * ROWS, 16), ROWS)
                            act(pltpu.make_async_copy(w.at[layer, own, few], w_in.at[:, here], sem_mv.at[2, n]))

    def start(copy):
        copy.start()

    def wait(copy):
        copy.wait()

    def load_a(src):
        return pltpu.make_async_copy(src, a_in, sem_a.at[0])

    def load_s(src):
        return pltpu.make_async_copy(src, s_in, sem_s.at[0])

    def tile(t, act):
        here = pl.ds(pl.multiple_of(t * SMALL, SMALL), SMALL)
        for n, src in enumerate((dg1, du1)):
            act(pltpu.make_async_copy(src.at[here, :], d_tile.at[n], sem_tile.at[n]))
        for n, src in enumerate((h1, dy)):
            act(pltpu.make_async_copy(src.at[here, :], h_tile.at[n], sem_tile.at[2 + n]))

    def hidden(n, act):
        here = pl.ds(pl.multiple_of((n // SIXTHS) * SMALL, SMALL), SMALL)
        cols = pl.ds(pl.multiple_of((n % SIXTHS) * NARROW, 128), NARROW)
        for m, src in enumerate((silu0, slope0)):
            act(pltpu.make_async_copy(src.at[here, cols], kept.at[n % AHEAD, m], sem_kept.at[n % AHEAD, m]))

    def back(t, act):
        here = pl.ds(pl.multiple_of(t * SMALL, SMALL), SMALL)
        for n, out in enumerate((dg0, du0)):
            act(pltpu.make_async_copy(d_tile.at[n], out.at[here, :], sem_d.at[n]))

    def load_w(n):
        src, dst = ((wg.at[1], wg_in), (wu.at[1], wu_in), (wd.at[0], wd_in))[n]
        return pltpu.make_async_copy(src, dst, sem_w.at[n])

    load_a(a1).start()
    operand(0, start)

    def step(i, carry):
        slot = i % 2

        @pl.when(i < CHUNKS)
        def _():
            operand(i, wait)

            @pl.when(i == 0)
            def _():
                load_a(a1).wait()
                tile(0, start)
                load_w(0).start()
                load_w(1).start()

            @pl.when(i == 1)
            def _():
                load_s(s1).start()

            @pl.when(i == 2)
            def _():
                load_w(2).start()
                for n in range(AHEAD):
                    hidden(n, start)

            @pl.when(i == 3)
            def _():
                load_s(s1).wait()

            @pl.when(i == 6)
            def _():
                load_s(s0).start()

            @pl.when(i == 9)
            def _():
                load_a(a0).start()
                load_s(s0).wait()

            @pl.when(i == 12)
            def _():
                load_a(a0).wait()

            @pl.when((i + 1 < CHUNKS) & (i != 11))
            def _():
                operand(i + 1, start)

            _, kind, _ = which(i)

            @pl.when(kind < 2)
            def _():
                term = dot(a_in[...], rhs[slot], TN).astype(BF16)
                part[slot] = term.reshape(2, 2, 2, 2, ROWS, WIDE)

            @pl.when(kind == 2)
            def _():
                for x in range(2):
                    term = dot(s_in[:, x * (FF // 2) : (x + 1) * (FF // 2)], rhs[slot, :, :256], TN).astype(BF16)
                    term = term.reshape(2, 2, 2, 4, ROWS, 256)
                    for n in range(4):
                        part[slot, x, :, :, :, :, pl.ds(256 * n, 256)] = term[:, :, :, n]

        @pl.when((i >= 5) & (i < 12))
        def _():
            back(i - 5, wait)

        @pl.when((i >= 1) & (i < 8))
        def _():
            tile(i, start)

        def stage(back, body):
            @pl.when((i >= back) & (i < CHUNKS + back))
            def _():
                body(i - back)

        @stage_with(stage, 8)
        def _(k):
            give4(k, wait)

        @stage_with(stage, 7)
        def _(k):
            give3(k, wait)
            give4(k, start)

        @stage_with(stage, 6)
        def _(k):
            give2(k, wait)
            give3(k, start)

        @stage_with(stage, 5)
        def _(k):
            state(k, wait, True)
            give1(k, wait)
            give2(k, start)

        @stage_with(stage, 4)
        def _(k):
            state(k, wait, False)
            for r in range(3):
                swap3(k, r).wait()
                mine = (k % 3, *pos, rows(r))
                total = (q[mine].astype(F32) + r3[k % 2, r].astype(F32)).astype(BF16).astype(F32)
                w, m, v = adamw(w_in[rows(r), :].astype(F32), m_in[rows(r), :], v_in[rows(r), :], total)
                m_out[rows(r), :] = m
                v_out[rows(r), :] = v
                new[rows(r), :] = w
                for n in range(4):
                    new_d[n, rows(r), :] = w[:, 256 * n : 256 * n + 256]
            give1(k, start)
            state(k, start, True)

        @stage_with(stage, 3)
        def _(k):
            state(k, start, False)
            for r in range(3):
                a, b = r, (r + 1) % 3
                swap2(k, r).wait()
                mine = (k % 3, *at({a: pos[a], b: pos[b]}), rows(r))
                q[mine] = (q[mine].astype(F32) + r2[k % 2, r].astype(F32)).astype(BF16)
            for r in range(3):
                swap3(k, r).start()

        @stage_with(stage, 2)
        def _(k):
            for r in range(3):
                swap1(k, r).wait()
                mine = (k % 3, *at({r: pos[r]}), rows(r))
                q[mine] = (q[mine].astype(F32) + r1[k % 2, r].astype(F32)).astype(BF16)
            for r in range(3):
                swap2(k, r).start()

        @stage_with(stage, 1)
        def _(k):
            swap0(k).wait()
            for n in range(2):
                mine = part[k % 2, n, :, :, core].astype(F32) + r0[k % 2, n].astype(F32)
                q[k % 3, n] = mine.astype(BF16)
            for r in range(3):
                swap1(k, r).start()

        @pl.when(i < CHUNKS)
        def _():
            swap0(i).start()

        @pl.when(i < 8)
        def _():
            tile(i, wait)

            @pl.when(i == 0)
            def _():
                load_w(0).wait()
                load_w(1).wait()

            d_a = dot(d_tile[0], wg_in[...], NT).astype(BF16) + dot(d_tile[1], wu_in[...], NT).astype(BF16)
            d_a = d_a.astype(F32)
            wide = h_tile[0].astype(F32)
            scale = scale_of(wide)
            along = jnp.mean(d_a * wide, -1, keepdims=True)
            d_h = (d_a * scale - wide * (scale * scale * scale * along)).astype(BF16)
            dh[pl.ds(pl.multiple_of(i * SMALL, SMALL), SMALL), :] = h_tile[1] + d_h

        @pl.when((i >= 4) & (i < 12))
        def _():
            @pl.when(i == 4)
            def _():
                load_w(2).wait()

            t = i - 4
            here = pl.ds(pl.multiple_of(t * SMALL, SMALL), SMALL)
            for p in range(SIXTHS):
                n = SIXTHS * t + p
                cols = slice(p * NARROW, (p + 1) * NARROW)
                hidden(n, wait)
                d_s = dot(dh[here, :], wd_in[cols, :], NT).astype(BF16).astype(F32)
                d_tile[0, :, cols] = (d_s * kept[n % AHEAD, 1] * 2).astype(BF16)
                d_tile[1, :, cols] = (d_s * kept[n % AHEAD, 0]).astype(BF16)

                @pl.when(n + AHEAD < 8 * SIXTHS)
                def _(n=n):
                    hidden(n + AHEAD, start)

            back(t, start)

        @pl.when(i == 11)
        def _():
            back(7, wait)
            operand(12, start)

        return carry

    lax.fori_loop(0, CHUNKS + 8, step, 0)


def stage_with(stage, back):
    return lambda body: stage(back, body)


def sum_and_step(ins, wg, wu, wd, mg, mu, md, vg, vu, vd):
    dims = (2, 2, 2, 2, 2)
    any_ = pl.BlockSpec(memory_space=pl.ANY)
    md, vd = (t.reshape(2, 4, ROWS, D) for t in (md, vd))
    vmem = pltpu.VMEM
    dma = pltpu.SemaphoreType.DMA
    outs = pl.pallas_call(
        sum_kernel,
        in_specs=[any_] * 19,
        out_specs=[any_] * 11,
        out_shape=[jax.ShapeDtypeStruct((*dims, ROWS, FF), BF16)] * 2
        + [jax.ShapeDtypeStruct((*dims, 4, ROWS, D), BF16)]
        + ([jax.ShapeDtypeStruct((2, ROWS, FF), F32)] * 2 + [jax.ShapeDtypeStruct((2, 4, ROWS, D), F32)]) * 2
        + [jax.ShapeDtypeStruct((TOKENS, FF), BF16)] * 2,
        scratch_shapes=[
            vmem((TOKENS, D), BF16),
            vmem((TOKENS, FF), BF16),
            vmem((2, TOKENS, WIDE), BF16),
            vmem((2, 2, 2, 2, 2, ROWS, WIDE), BF16),
            vmem((2, 2, 2, 2, ROWS, WIDE), BF16),
            vmem((3, 2, 2, 2, ROWS, WIDE), BF16),
            vmem((2, 3, 2, 2, 16, WIDE), BF16),
            vmem((2, 3, 2, 16, WIDE), BF16),
            vmem((2, 3, 16, WIDE), BF16),
            vmem((ROWS, WIDE), BF16),
            vmem((4, ROWS, 256), BF16),
            vmem((ROWS, WIDE), F32),
            vmem((ROWS, WIDE), F32),
            vmem((ROWS, WIDE), BF16),
            vmem((ROWS, WIDE), F32),
            vmem((ROWS, WIDE), F32),
            vmem((D, FF), BF16),
            vmem((D, FF), BF16),
            vmem((FF, D), BF16),
            vmem((TOKENS, D), BF16),
            vmem((2, SMALL, FF), BF16),
            vmem((2, SMALL, D), BF16),
            vmem((AHEAD, 2, SMALL, NARROW), F32),
            dma((1,)),
            dma((1,)),
            dma((2,)),
            dma((3, 4)),
            dma((2, 4)),
            dma((1,)),
            dma((2, 2)),
            *[dma((2, 2, 3))] * 6,
            dma((2, 2)),
            dma((3,)),
            dma((4,)),
            dma((AHEAD, 2)),
            dma((2,)),
        ],
        compiler_params=pltpu.CompilerParams(collective_id=0, has_side_effects=True, vmem_limit_bytes=67043328),
        cost_estimate=pl.CostEstimate(flops=9 * 2 * TOKENS * D * FF, bytes_accessed=120 * MIB, transcendentals=0),
    )(*ins, wg, wu, wd, mg, mu, md, vg, vu, vd)
    shapes = [(2, D, FF)] * 2 + [(2, FF, D)] + ([(2, ROWS, FF)] * 2 + [(2, 4 * ROWS, D)]) * 2
    return copied([t.reshape(shape) for t, shape in zip(outs[:9], shapes, strict=True)])


def copy_kernel(*refs):
    n = len(refs) // 2
    for src, dst in zip(refs[:n], refs[n:], strict=True):
        dst[...] = src[...]


def copied(arrays):
    specs = [pl.BlockSpec((None, t.shape[1] // COPIES, t.shape[2]), lambda i: (i // COPIES, i % COPIES, 0)) for t in arrays]
    return tuple(
        pl.pallas_call(
            copy_kernel,
            grid=(2 * COPIES,),
            in_specs=specs,
            out_specs=specs,
            out_shape=[jax.ShapeDtypeStruct(t.shape, t.dtype) for t in arrays],
            compiler_params=pltpu.CompilerParams(vmem_limit_bytes=62 * MIB),
        )(*arrays)
    )


def solution(mesh):
    def step(x, dy, wg, wu, wd, *moments):
        x, dy = x[0], dy[0]
        weights = wg, wu, wd
        kept = (D, BF16), (FF, F32), (FF, F32), (FF, BF16), (D, BF16)
        a0, silu0, slope0, s0, h1 = by_columns(forward_kernel, (x,), weights, 0, kept, True, [pltpu.VMEM((TOKENS, FF), BF16)])
        made = (D, BF16), (FF, BF16), (FF, BF16), (FF, BF16)
        a1, s1, dg1, du1 = by_columns(turn_kernel, (h1, dy), weights, 1, made, False, [])
        return sum_and_step((a1, a0, s1, s0, dy, h1, dg1, du1, silu0, slope0), wg, wu, wd, *moments)

    whole, rows = P(None, None, None), P(None, "dp", None)
    return jax.shard_map(
        step,
        mesh=mesh,
        in_specs=(P(("rep", "dp")), P(("rep", "dp")), *[whole] * 3, *[rows] * 6),
        out_specs=(*[P("rep", None, None)] * 3, *[P("rep", "dp", None)] * 6),
        check_vma=False,
    )
```
